16 devices in a mesh: dp: 4 (over z, y), ep: 4 (over x, core).
Axes of the slice: x: 2, y: 2, z: 2, core: 2. Of those that a mesh axis runs over, the one named last changes fastest.
Arguments:
- x: bfloat16 [131072, 1024], P(('dp', 'ep'))
- gy: bfloat16 [131072, 1024], P(('dp', 'ep'))
- idx: int32 [131072], P(('dp', 'ep'))
- w_gate: bfloat16 [1024, 32], replicated
- w_up: bfloat16 [32, 1024, 512], P('ep')
- w_down: bfloat16 [32, 512, 1024], P('ep')
Outputs:
- output 1: bfloat16 [131072, 1024], P(('dp', 'ep'))
- output 2: bfloat16 [131072, 1024], P(('dp', 'ep'))
- output 3: float32 [32, 1024, 512], P('ep')
- output 4: float32 [32, 512, 1024], P('ep')
- output 5: float32 [1024, 32], replicated
All inputs are finite; a program needn't handle non-finite values.
Results may differ from the reference program's by a relative error of at most 0.00656889.
Values are sent between devices in bfloat16 or wider.
A program may use at most 1 GiB of HBM per device.

```python
import functools
import jax
import jax.numpy as jnp
from jax import lax

D_MODEL = 1024
D_FF = 512
N_EXPERTS = 32
TOKENS_DEV = 8192
N_DEVICES = 16
TILE_ROWS = 128
N_TOKENS = N_DEVICES * TOKENS_DEV
CAP_ROWS = 4 * TOKENS_DEV // N_EXPERTS
N_TILES = N_TOKENS // TILE_ROWS + N_EXPERTS


def count_profile():
    hot_experts = max(1, N_EXPERTS // 16)
    cold_experts = N_EXPERTS - hot_experts
    rest_rows = TOKENS_DEV - hot_experts * CAP_ROWS
    base_rows = rest_rows // cold_experts
    extra_rows = rest_rows % cold_experts
    return [CAP_ROWS] * hot_experts + [base_rows + 1] * extra_rows + [base_rows] * (cold_experts - extra_rows)


def draw_routing(route_key):
    profile = count_profile()
    rank_table = jnp.array([rank_id for rank_id in range(N_EXPERTS) for copy_num in range(profile[rank_id])], jnp.int32)

    def one_device(dev_key):
        perm_key, shuffle_key = jax.random.split(dev_key)
        expert_perm = jax.random.permutation(perm_key, N_EXPERTS).astype(jnp.int32)
        return jax.random.permutation(shuffle_key, expert_perm[rank_table])

    return jax.vmap(one_device)(jax.random.split(route_key, N_DEVICES)).reshape(N_TOKENS)


def setup_inputs(seed: int = 0) -> dict:
    root_key = jax.random.key(seed)
    k_x, k_gy, k_gate, k_up, k_down, k_route = jax.random.split(root_key, 6)
    x = jax.random.normal(k_x, (N_TOKENS, D_MODEL), jnp.float32).astype(jnp.bfloat16)
    gy = jax.random.normal(k_gy, (N_TOKENS, D_MODEL), jnp.float32).astype(jnp.bfloat16)
    w_gate = (jax.random.normal(k_gate, (D_MODEL, N_EXPERTS), jnp.float32) * D_MODEL ** -0.5).astype(jnp.bfloat16)
    w_up = (jax.random.normal(k_up, (N_EXPERTS, D_MODEL, D_FF), jnp.float32) * D_MODEL ** -0.5).astype(jnp.bfloat16)
    w_down = (jax.random.normal(k_down, (N_EXPERTS, D_FF, D_MODEL), jnp.float32) * D_FF ** -0.5).astype(jnp.bfloat16)
    idx = draw_routing(k_route)
    return {'x': x, 'gy': gy, 'idx': idx, 'w_gate': w_gate, 'w_up': w_up, 'w_down': w_down}


def tile_pass(w_up, w_down, grad_carry, tile_in):
    grad_up, grad_down = grad_carry
    tok_rows, d_out, expert = tile_in
    up_mat = w_up[expert]
    down_mat = w_down[expert]
    pre_act = jnp.dot(tok_rows, up_mat, preferred_element_type=jnp.float32)
    hid_full, gelu_back = jax.vjp(jax.nn.gelu, pre_act)
    hidden = hid_full.astype(jnp.bfloat16)
    y_rows = jnp.dot(hidden, down_mat, preferred_element_type=jnp.float32).astype(jnp.bfloat16)
    d_hidden = jnp.dot(d_out, down_mat.T, preferred_element_type=jnp.float32)
    d_pre = gelu_back(d_hidden)[0].astype(jnp.bfloat16)
    grad_down = grad_down.at[expert].add(jnp.dot(hidden.T, d_out, preferred_element_type=jnp.float32))
    grad_up = grad_up.at[expert].add(jnp.dot(tok_rows.T, d_pre, preferred_element_type=jnp.float32))
    d_rows = jnp.dot(d_pre, up_mat.T, preferred_element_type=jnp.float32).astype(jnp.bfloat16)
    return (grad_up, grad_down), (y_rows, d_rows)


def reference(x, gy, idx, w_gate, w_up, w_down):
    onehot = idx[:, None] == jnp.arange(N_EXPERTS, dtype=jnp.int32)[None, :]
    router_logit = jnp.dot(x, w_gate, preferred_element_type=jnp.float32)
    router_prob = jax.nn.softmax(router_logit, axis=-1)
    gate_val = N_EXPERTS * jnp.sum(jnp.where(onehot, router_prob, 0.0), axis=1)
    expert_count = jnp.sum(onehot, axis=0, dtype=jnp.int32)
    sort_order = jnp.argsort(idx, stable=True)
    sorted_pos = jnp.argsort(sort_order)
    expert_start = jnp.cumsum(expert_count) - expert_count
    tile_count = (expert_count + TILE_ROWS - 1) // TILE_ROWS * TILE_ROWS
    tile_end = jnp.cumsum(tile_count)
    tile_start = tile_end - tile_count
    row_pos = tile_start[idx] + sorted_pos - expert_start[idx]
    tile_first = jnp.arange(N_TILES, dtype=jnp.int32) * TILE_ROWS
    tile_expert = jnp.minimum(jnp.sum(tile_end[None, :] <= tile_first[:, None], axis=1, dtype=jnp.int32), N_EXPERTS - 1)
    gy_full = gy.astype(jnp.float32)
    dy_tok = (gate_val[:, None] * gy_full).astype(jnp.bfloat16)
    rows_buf = jnp.zeros((N_TILES * TILE_ROWS, D_MODEL), x.dtype).at[row_pos].set(x)
    dy_buf = jnp.zeros((N_TILES * TILE_ROWS, D_MODEL), dy_tok.dtype).at[row_pos].set(dy_tok)
    grad_init = (jnp.zeros((N_EXPERTS, D_MODEL, D_FF), jnp.float32), jnp.zeros((N_EXPERTS, D_FF, D_MODEL), jnp.float32))
    tiles_in = (rows_buf.reshape(N_TILES, TILE_ROWS, D_MODEL), dy_buf.reshape(N_TILES, TILE_ROWS, D_MODEL), tile_expert)
    grads, tile_out = lax.scan(functools.partial(tile_pass, w_up, w_down), grad_init, tiles_in)
    grad_up, grad_down = grads
    y_tok = tile_out[0].reshape(N_TILES * TILE_ROWS, D_MODEL)[row_pos]
    dx_expert = tile_out[1].reshape(N_TILES * TILE_ROWS, D_MODEL)[row_pos]
    moe_out = (gate_val[:, None] * y_tok.astype(jnp.float32)).astype(jnp.bfloat16)
    d_gate = jnp.sum(gy_full * y_tok.astype(jnp.float32), axis=1)
    d_logit = ((d_gate * gate_val)[:, None] * (onehot.astype(jnp.float32) - router_prob)).astype(jnp.bfloat16)
    dx_router = jnp.dot(d_logit, w_gate.T, preferred_element_type=jnp.float32)
    grad_x = (dx_expert.astype(jnp.float32) + dx_router).astype(jnp.bfloat16)
    grad_gate = jnp.dot(x.T, d_logit, preferred_element_type=jnp.float32)
    return (moe_out, grad_x, grad_up, grad_down, grad_gate)
```

```python
import functools

import jax
import jax.numpy as jnp
from jax import lax
from jax.experimental import pallas as pl
from jax.experimental.pallas import tpu as pltpu
from jax.sharding import PartitionSpec as P

ROWS = 256
ALIGN = 16
PIECES = (256, 128, 64, 32, 16)
GELU_C = 0.7978845608028654
GELU_A = 0.044715


def chunk_tables(counts, starts):
    calls, n_exp = counts.shape
    cap = n_exp * (1024 // ROWS)
    per = (counts + ROWS - 1) // ROWS
    end = jnp.cumsum(per, axis=1)
    begin = end - per
    c = jnp.arange(cap, dtype=jnp.int32)
    e = jnp.sum((c[None, :, None] >= end[:, None, :]).astype(jnp.int32), axis=2)
    hot = (e[:, :, None] == jnp.arange(n_exp, dtype=jnp.int32)).astype(jnp.int32)
    pick = lambda v: jnp.sum(hot * v[:, None, :], axis=2)
    j = c[None, :] - pick(begin)
    start = pick(starts) + j * ROWS
    n = jnp.clip(pick(counts) - j * ROWS, 0, ROWS)
    bounds = jnp.concatenate([begin, jnp.broadcast_to(end[:, -1:], (calls, cap - n_exp))], axis=1)
    return jnp.stack([jnp.where(n > 0, start, 0), n, bounds], axis=1)


def ffn_kernel(n_init, has_prev, tab, x_hbm, dy_hbm, w1, w2, *rest):
    rest = list(rest)
    inits = rest[: 2 * n_init]
    rest = rest[2 * n_init:]
    if has_prev:
        rest = rest[2:]
    dw1, dw2, y_hbm, dx_hbm, xb, dyb, yb, dxb, isem, osem = rest
    e = pl.program_id(0)
    n_exp = pl.num_programs(0)
    total = tab[2, n_exp]

    def pieces(ci, body):
        start = tab[0, ci]
        n = tab[1, ci]
        rows = (n + ALIGN - 1) & -ALIGN
        off = jnp.int32(0)
        for size in PIECES:
            has = (rows & size) != 0

            @pl.when(has)
            def _(off=off, size=size):
                body(pl.ds(pl.multiple_of(start + off, ALIGN), size), pl.ds(pl.multiple_of(off, ALIGN), size))

            off = off + jnp.where(has, size, 0)

    def load(ci, sl, act):
        def body(h, v):
            act(pltpu.make_async_copy(x_hbm.at[h], xb.at[sl, v], isem.at[0, sl]))
            act(pltpu.make_async_copy(dy_hbm.at[h], dyb.at[sl, v], isem.at[1, sl]))
        pieces(ci, body)

    def store(ci, sl, act):
        def body(h, v):
            act(pltpu.make_async_copy(yb.at[sl, v], y_hbm.at[h], osem.at[0, sl]))
            act(pltpu.make_async_copy(dxb.at[sl, v], dx_hbm.at[h], osem.at[1, sl]))
        pieces(ci, body)

    start_op = lambda d: d.start()
    wait_op = lambda d: d.wait()

    @pl.when((e == 0) & (total > 0))
    def _():
        load(0, 0, start_op)

    if n_init == 2:
        dw1[...] = inits[0][...] + inits[2][...]
        dw2[...] = inits[1][...] + inits[3][...]
    elif n_init == 1:
        dw1[...] = inits[0][...]
        dw2[...] = inits[1][...]
    else:
        dw1[...] = jnp.zeros_like(dw1)
        dw2[...] = jnp.zeros_like(dw2)

    @pl.loop(tab[2, e], tab[2, e + 1])
    def _(c):
        slot = lax.rem(c, 2)

        @pl.when(c + 1 < total)
        def _():
            load(c + 1, 1 - slot, start_op)

        load(c, slot, wait_op)

        @pl.when(c >= 2)
        def _():
            store(c - 2, slot, wait_op)

        keep = lax.broadcasted_iota(jnp.int32, (ROWS, 1), 0) < tab[1, c]
        x = jnp.where(keep, xb[slot], jnp.zeros((), jnp.bfloat16))
        dy = jnp.where(keep, dyb[slot], jnp.zeros((), jnp.bfloat16))
        a = jnp.dot(x, w1[0], preferred_element_type=jnp.float32)
        a2 = a * a
        t = jnp.tanh(GELU_C * (a + GELU_A * (a2 * a)))
        cdf = 0.5 * (1.0 + t)
        h = (a * cdf).astype(jnp.bfloat16)
        yb[slot] = jnp.dot(h, w2[0], preferred_element_type=jnp.float32).astype(jnp.bfloat16)
        dh = lax.dot_general(dy, w2[0], (((1,), (1,)), ((), ())), preferred_element_type=jnp.float32)
        slope = cdf + 0.5 * a * ((1.0 - t * t) * (GELU_C * (1.0 + 3.0 * GELU_A * a2)))
        da = (dh * slope).astype(jnp.bfloat16)
        dxb[slot] = lax.dot_general(da, w1[0], (((1,), (1,)), ((), ())), preferred_element_type=jnp.float32).astype(jnp.bfloat16)
        store(c, slot, start_op)
        dw2[0] += lax.dot_general(h, dy, (((0,), (0,)), ((), ())), preferred_element_type=jnp.float32)
        dw1[0] += lax.dot_general(x, da, (((0,), (0,)), ((), ())), preferred_element_type=jnp.float32)

    @pl.when(e == n_exp - 1)
    def _():
        for back in (2, 1):
            @pl.when(total >= back)
            def _(back=back):
                store(total - back, lax.rem(total - back, 2), wait_op)


def ffn(tab, x, dy, w1, w2, init=(), prev=None):
    n_rows, d = x.shape
    n_exp, _, f = w1.shape
    per_expert = lambda e, t: (e, 0, 0)
    any_spec = pl.BlockSpec(memory_space=pl.ANY)
    w_specs = [pl.BlockSpec((1, d, f), per_expert), pl.BlockSpec((1, f, d), per_expert)]
    args = [x, dy, w1, w2]
    specs = [any_spec, any_spec] + w_specs
    alias = {}
    if init:
        alias.update({1 + len(args): 0, 2 + len(args): 1})
    for pair in init:
        args += list(pair)
        specs += w_specs
    if prev is not None:
        alias.update({1 + len(args): 2, 2 + len(args): 3})
        args += list(prev)
        specs += [any_spec, any_spec]
    return pl.pallas_call(
        functools.partial(ffn_kernel, len(init), prev is not None),
        grid_spec=pltpu.PrefetchScalarGridSpec(
            num_scalar_prefetch=1,
            grid=(n_exp,),
            in_specs=specs,
            out_specs=w_specs + [any_spec, any_spec],
            scratch_shapes=[pltpu.VMEM((2, ROWS, d), jnp.bfloat16)] * 4 + [pltpu.SemaphoreType.DMA((2, 2))] * 2,
        ),
        out_shape=[
            jax.ShapeDtypeStruct((n_exp, d, f), jnp.float32),
            jax.ShapeDtypeStruct((n_exp, f, d), jnp.float32),
            jax.ShapeDtypeStruct((n_rows, d), jnp.bfloat16),
            jax.ShapeDtypeStruct((n_rows, d), jnp.bfloat16),
        ],
        input_output_aliases=alias,
        compiler_params=pltpu.CompilerParams(dimension_semantics=("arbitrary",), vmem_limit_bytes=58 * 1024 * 1024),
        cost_estimate=pl.CostEstimate(flops=12 * 4096 * d * f, bytes_accessed=96 * 1024 * 1024, transcendentals=4096 * f),
    )(tab, *args)


def solution(mesh):
    tok_spec = P(('dp', 'ep'), None)
    idx_spec = P(('dp', 'ep'))
    rep_spec = P(None, None)
    exp_spec = P('ep', None, None)
    ep_size = mesh.shape['ep']
    swap_x = [(i, i ^ 2) for i in range(ep_size)]
    swap_core = [(i, i ^ 1) for i in range(ep_size)]

    def local_step(x_loc, gy_loc, idx_loc, w_gate, w_up, w_down):
        tok, d = x_loc.shape
        n_exp = w_gate.shape[1]
        per_dev = w_up.shape[0]
        half = n_exp // 2
        slots = tok + n_exp * ALIGN
        levels = (4960, tok + half * ALIGN)
        ep = lax.axis_index('ep')
        dp = lax.axis_index('dp')
        w_up_s = lax.ppermute(w_up, 'ep', swap_core)
        w_down_s = lax.ppermute(w_down, 'ep', swap_core)

        key = ((idx_loc // per_dev) ^ (ep ^ 1)) * per_dev + idx_loc % per_dev
        lanes = jnp.arange(n_exp, dtype=jnp.int32)
        count = jnp.sum((key[:, None] == lanes[None, :]).astype(jnp.int32), axis=0)
        all_count = lax.all_gather(count, ('dp', 'ep'))

        def gap(k):
            return jnp.where(k >= half, k + 1, k)

        fill = jnp.arange(ALIGN, dtype=jnp.int32)
        fill_cls = jnp.where(fill[None, :] < ((-count) % ALIGN)[:, None], gap(lanes)[:, None], half).reshape(-1)
        cls = jnp.concatenate([gap(key), fill_cls])
        ids = jnp.arange(slots, dtype=jnp.int32)
        order = lax.sort(cls * 16384 + ids, is_stable=False) % 16384
        slot_of = lax.sort(order * 16384 + ids, is_stable=False)[:tok] % 16384
        src = jnp.where(order < tok, order, 0)
        xs = x_loc[src]

        logit = jnp.dot(x_loc, w_gate, preferred_element_type=jnp.float32)
        prob = jax.nn.softmax(logit, axis=-1)
        onehot = idx_loc[:, None] == lanes[None, :]
        gate = n_exp * jnp.sum(jnp.where(onehot, prob, 0.0), axis=1)
        dy = (gate[:, None] * gy_loc.astype(jnp.float32)).astype(jnp.bfloat16)
        dys = dy[src]

        def padded(cnt):
            return (cnt + ALIGN - 1) // ALIGN * ALIGN

        all_pad = padded(all_count)
        tail_need = jnp.max(jnp.sum(all_pad[:, half:], axis=1))
        level = sum((tail_need > c).astype(jnp.int32) for c in levels[:-1])
        pad_own = padded(count)
        head_start = jnp.cumsum(pad_own[:half]) - pad_own[:half]
        head_total = jnp.sum(pad_own[:half])
        p_count = lax.dynamic_index_in_dim(all_count, dp * ep_size + (ep ^ 2), 0, keepdims=False)[half:]
        p_pad = padded(p_count)
        tail_start = jnp.cumsum(p_pad) - p_pad - jnp.sum(p_pad)

        def run(cap, ops):
            xs, dys, slot_of, head_start, tail_start, count, p_count, w_up, w_down, w_up_s, w_down_s, x_loc, gy_loc, gate, prob, onehot, w_gate = ops
            rx = lax.ppermute(xs[slots - cap:], 'ep', swap_x)
            rdy = lax.ppermute(dys[slots - cap:], 'ep', swap_x)
            k = per_dev
            tab = chunk_tables(
                jnp.stack([count[:k], count[k:2 * k], p_count[:k], p_count[k:]]),
                jnp.stack([head_start[:k], head_start[k:], cap + tail_start[:k], cap + tail_start[k:]]),
            )
            dws1, dws2, yo, dxo = ffn(tab[0], xs, dys, w_up_s, w_down_s)
            dws1, dws2, yp, dxp = ffn(tab[2], rx, rdy, w_up_s, w_down_s, init=((dws1, dws2),))
            add1 = lax.ppermute(dws1, 'ep', swap_core)
            add2 = lax.ppermute(dws2, 'ep', swap_core)
            dwo1, dwo2, yo, dxo = ffn(tab[1], xs, dys, w_up, w_down, prev=(yo, dxo))
            dwo1, dwo2, yp, dxp = ffn(tab[3], rx, rdy, w_up, w_down, init=((dwo1, dwo2), (add1, add2)), prev=(yp, dxp))
            ry = lax.ppermute(yp, 'ep', swap_x)
            rdx = lax.ppermute(dxp, 'ep', swap_x)
            g_up = lax.psum(dwo1, 'dp')
            g_down = lax.psum(dwo2, 'dp')
            gy_full = gy_loc.astype(jnp.float32)
            in_head = (jnp.arange(slots, dtype=jnp.int32) < head_total)[:, None]
            merge = lambda own, ret: jnp.where(in_head, own, jnp.pad(ret, ((slots - cap, 0), (0, 0))))
            y_tok = merge(yo, ry)[slot_of].astype(jnp.float32)
            moe_out = (gate[:, None] * y_tok).astype(jnp.bfloat16)
            d_gate = jnp.sum(gy_full * y_tok, axis=1)
            d_logit = ((d_gate * gate)[:, None] * (onehot.astype(jnp.float32) - prob)).astype(jnp.bfloat16)
            g_gate = jnp.einsum('td,te->de', x_loc, d_logit, preferred_element_type=jnp.float32)
            for axis, flip in (('ep', 1), ('ep', 2), ('dp', 1), ('dp', 2)):
                g_gate = g_gate + lax.ppermute(g_gate, axis, [(i, i ^ flip) for i in range(mesh.shape[axis])])
            dx_exp = merge(dxo, rdx)[slot_of]
            dx_router = jnp.einsum('te,de->td', d_logit, w_gate, preferred_element_type=jnp.float32)
            g_x = (dx_exp.astype(jnp.float32) + dx_router).astype(jnp.bfloat16)
            return moe_out, g_x, g_up, g_down, g_gate

        ops = (xs, dys, slot_of, head_start, tail_start, count, p_count, w_up, w_down, w_up_s, w_down_s, x_loc, gy_loc, gate, prob, onehot, w_gate)
        return lax.switch(level, [functools.partial(run, c) for c in levels], ops)

    return jax.shard_map(local_step, mesh=mesh, in_specs=(tok_spec, tok_spec, idx_spec, rep_spec, exp_spec, exp_spec), out_specs=(tok_spec, tok_spec, exp_spec, exp_spec, rep_spec), check_vma=False)
```
